32 devices in a mesh: dp: 4 (over y, core), tensor: 2 (over x), pipe: 4 (over z).
Axes of the slice: x: 2, y: 2, z: 4, core: 2. Of those that a mesh axis runs over, the one named last changes fastest.
Arguments:
- grad_parts: float32 [4, 4, 2, 64, 8192], P('dp', 'pipe', 'tensor'), may hold values from -24 to 24
- drop_flags: int32 [4, 4, 2, 64], P('dp', 'pipe', 'tensor'), may hold values from 0 to 1, as said below
- owner_order: int32 [4], replicated, may hold values from 0 to 3, each once
- step_count: int32 [], replicated, may hold values from 1 to 11
- master: float32 [4, 2, 64, 8192], P('pipe', 'tensor', None, 'dp'), may hold values from -6 to 6
- moment_m: float32 [4, 2, 64, 8192], P('pipe', 'tensor', None, 'dp'), may hold values from -0.15625 to 0.15625
- moment_v: float32 [4, 2, 64, 8192], P('pipe', 'tensor', None, 'dp'), may hold values from 0.0001 to 0.001
Outputs:
- new_master: float32 [4, 2, 64, 8192], P('pipe', 'tensor', None, 'dp')
- new_m: float32 [4, 2, 64, 8192], P('pipe', 'tensor', None, 'dp')
- new_v: float32 [4, 2, 64, 8192], P('pipe', 'tensor', None, 'dp')
- direction: float32 [4, 2, 64, 8192], P('pipe', 'tensor', None, 'dp')
- dropped_total: int32 [], replicated
The draws below stay inside these ranges and needn't reach their ends.
Inputs may be any that keep to these rules, and one draw needn't show every extreme that they name: `drop_flags`: A row may be flagged by every replica.
All inputs are finite; a program needn't handle non-finite values.
Results may differ from the reference program's by a relative error of at most 0.0003.
Values sent between devices are 32-bit elements; how exact they have to be, the bound alone decides.
A program may use at most 64 MiB of HBM per device.

```python
import math
import jax
import jax.numpy as jnp
from jax import lax

D = 8192
ROWS = 64
LAYERS = 4
SHARDS = 2
N_DP = 4


def draw_drop_flags(key, part):
    random_ones = jax.random.randint(jax.random.fold_in(key, 11), (N_DP, LAYERS, SHARDS, ROWS), 0, 4) == 0
    full_rows = jax.random.randint(jax.random.fold_in(key, 12), (LAYERS, SHARDS, ROWS), 0, 32) == 0
    forced = jax.random.randint(jax.random.fold_in(key, 13), (), 0, LAYERS * SHARDS * ROWS)
    position = jnp.arange(LAYERS * SHARDS * ROWS, dtype=jnp.int32).reshape(LAYERS, SHARDS, ROWS)
    every_replica = full_rows | (position == forced)
    return jnp.where(random_ones | every_replica[None], 1, 0).astype(jnp.int32)


def draw_grad_parts(key, part):
    block_cols = D // N_DP
    pairing = jax.random.permutation(jax.random.fold_in(key, 21), N_DP)
    column_block = jnp.arange(D, dtype=jnp.int32) // block_cols
    spiked = column_block[None, :] == pairing[:, None]
    factor = jnp.where(spiked, 4.0, 1.0).astype(jnp.float32)[:, None, None, None, :]
    noise = jax.random.normal(jax.random.fold_in(key, 22), (N_DP, LAYERS, SHARDS, ROWS, D), jnp.float32)
    own_part = jnp.clip(noise, -6.0, 6.0) * factor
    values = own_part
    return values.astype(jnp.float32)


def levels(own_key, dims, pieces, low, top_value):
    gain = 1.0
    for axis_at, shards_of in pieces:
        heights = jax.random.uniform(jax.random.fold_in(jax.random.fold_in(own_key, 6), axis_at), (shards_of,), jnp.float32, low / len(pieces), top_value / len(pieces))
        gain = gain * jnp.repeat(jnp.exp(heights), dims[axis_at] // shards_of).reshape((-1,) + (1,) * (len(dims) - 1 - axis_at))
    return gain


def gaussian(key, shape, spread, most, pieces=(), kind=jnp.bfloat16):
    array = jax.random.normal(key, shape, jnp.float32) * spread
    if len(pieces) > 0:
        array = levels(key, shape, pieces, -0.22, 0.18) * array
    return jnp.clip(array, min=-most, max=most).astype(kind)


def setup_inputs(seed: int = 0) -> dict:
    streams_of = jax.random.split(jax.random.key(seed), 8)
    return {
        "grad_parts": draw_grad_parts(jax.random.fold_in(streams_of[7], 71), 0),
        "drop_flags": draw_drop_flags(jax.random.fold_in(streams_of[7], 71), 0),
        "owner_order": jax.random.permutation(streams_of[2], N_DP).astype(jnp.int32),
        "step_count": jax.random.randint(streams_of[3], (), 1, 12).astype(jnp.int32),
        "master": gaussian(streams_of[4], (LAYERS, SHARDS, ROWS, D), 1.0, 6.0, ((0, 4), (1, 2), (3, 4)), jnp.float32),
        "moment_m": gaussian(streams_of[5], (LAYERS, SHARDS, ROWS, D), 0.01, 0.15625, ((0, 4), (1, 2), (3, 4)), jnp.float32),
        "moment_v": jnp.clip(jnp.exp(math.log(0.001) - 2.3025852 * jax.random.uniform(streams_of[6], (LAYERS, SHARDS, ROWS, D), jnp.float32) ** levels(streams_of[6], (LAYERS, SHARDS, ROWS, D), ((0, 4), (1, 2), (3, 4)), -0.2, 0.2)), 0.0001, 0.001),
    }


def reference(grad_parts, drop_flags, owner_order, step_count, master, moment_m, moment_v):
    kept = (1 - drop_flags).astype(jnp.float32)

    def accumulate(carry, pair):
        part, keep = pair
        return ((carry[0] + part * keep[..., None], carry[1] + keep), None)
    start = (jnp.zeros(grad_parts.shape[1:], jnp.float32), jnp.zeros(kept.shape[1:], jnp.float32))
    (total, count), unused = lax.scan(accumulate, start, (grad_parts, kept))
    mean_grad = total / jnp.maximum(count, 1.0)[..., None]
    shape = mean_grad.shape
    blocks = mean_grad.reshape(shape[0], shape[1], shape[2], N_DP, shape[3] // N_DP)
    grad = jnp.take(blocks, owner_order, axis=3).reshape(shape)
    entries = shape[0] * shape[1] * shape[2] * shape[3]
    rms = jnp.sqrt(jnp.sum(grad * grad) / entries)
    clip = jnp.minimum(1.0, 0.05 / (rms + 1e-06))
    scaled = clip * grad
    new_m = 0.9 * moment_m + 0.1 * scaled
    new_v = 0.999 * moment_v + 0.001 * scaled * scaled
    steps = step_count.astype(jnp.float32)
    m_hat = new_m / (1.0 - jnp.power(0.9, steps))
    v_hat = new_v / (1.0 - jnp.power(0.999, steps))
    direction = m_hat / (jnp.sqrt(v_hat) + 1e-08) + 0.1 * master
    new_master = master - 0.001 * direction
    dropped_total = jnp.sum(drop_flags).astype(jnp.int32)
    return (new_master, new_m, new_v, direction, dropped_total)
```

```python
import functools
import itertools
import jax
import jax.numpy as jnp
from jax import lax
from jax.experimental import pallas as pl
from jax.experimental.pallas import tpu as pltpu
from jax.sharding import PartitionSpec as P

AXES = ("dp", "tensor", "pipe")
MESH = pl.DeviceIdType.MESH
LANES = 128
DIRECT = 64


def as_column(row, rows):
    square = (rows, rows)
    diagonal = lax.broadcasted_iota(jnp.int32, square, 0) == lax.broadcasted_iota(jnp.int32, square, 1)
    return jnp.sum(jnp.where(diagonal, jnp.broadcast_to(row, square), 0.0), axis=1, keepdims=True)


def int_power(base, exponent):
    result = jnp.ones(exponent.shape, jnp.float32)
    square = jnp.full(exponent.shape, base, jnp.float32)
    for bit in range(31):
        result = jnp.where((exponent >> bit) & 1 == 1, result * square, result)
        square = square * square
    return result


def kernel(
    sizes, stages, entries, chunks,
    order_ref, step_ref, flags_ref, grad_hbm, w_hbm, m_hbm, v_hbm,
    w_out, m_out, v_out, dir_out, drop_out,
    g_bufs, w_buf, m_buf, v_buf, pair_send, pair_recv, ring_send, ring_recv,
    kept_send, kept_recv, total, red_sends, red_recvs,
    g_sem, st_sem, ps_sem, pr_sem, rs_sem, rr_sem, ks_sem, kr_sem, as_sems, ar_sems,
):
    n = sizes["dp"]
    chips = n // 2
    rows, width = w_buf.shape
    part = rows // chunks
    me = {axis: lax.axis_index(axis) for axis in AXES}
    chip, core = lax.div(me["dp"], 2), lax.rem(me["dp"], 2)

    def peer(offsets):
        return {axis: lax.rem(me[axis] + off, sizes[axis]) for axis, off in offsets.items()}

    def offsets_of(axes):
        ranges = [range(sizes[axis]) for axis in axes]
        return [dict(zip(axes, offs)) for offs in itertools.product(*ranges) if any(offs)]

    loads = []
    for k in range(chunks):
        copy = pltpu.make_async_copy(grad_hbm.at[0, 0, 0, pl.ds(k * part, part)], g_bufs[k], g_sem.at[k])
        copy.start()
        loads.append(copy)
    states = [
        pltpu.make_async_copy(src.at[0, 0], dst, st_sem.at[i])
        for i, (src, dst) in enumerate(((w_hbm, w_buf), (m_hbm, m_buf), (v_hbm, v_buf)))
    ]
    for copy in states:
        copy.start()

    barrier = pltpu.get_barrier_semaphore()
    friends = [tuple(sorted(off.items())) for axes in stages for off in offsets_of(axes)]
    friends += [tuple(sorted(off.items())) for off in offsets_of(("dp",))]
    full = [tuple(sorted({**dict.fromkeys(AXES, 0), **dict(off)}.items())) for off in friends]
    full = list(dict.fromkeys(full))
    for off in full:
        pl.semaphore_signal(barrier, inc=1, device_id=peer(dict(off)), device_id_type=MESH)

    flags_row = flags_ref[0].astype(jnp.float32)
    kept_row = 1.0 - flags_row
    kept = as_column(kept_row, rows)
    kept_send[0, :, 0:rows] = kept_row
    dropped = jnp.sum(flags_row, axis=1, keepdims=True)

    def chip_at(slot):
        return lax.rem(chip + slot, chips)

    def term(k, owner):
        block = order_ref[owner]
        picked = None
        for b in range(n):
            weight = (1 - jnp.minimum(jnp.maximum(block - b, b - block), 1)).astype(jnp.float32)
            piece = g_bufs[k][:, b * width:(b + 1) * width] * weight
            picked = piece if picked is None else picked + piece
        return picked * kept[k * part:(k + 1) * part]

    slots = list(range(1, chips)) + [0]
    for k in range(chunks):
        loads[k].wait()
        for slot in slots:
            pair_send[k, slot] = term(k, chip_at(slot) * 2 + 1 - core)

    pl.semaphore_wait(barrier, len(full))

    sibling = {"dp": chip * 2 + 1 - core}
    pair, waits = {}, []
    for group in (slots[:-1], slots[-1:]):
        for k in range(chunks):
            for slot in group:
                copy = pltpu.make_async_remote_copy(
                    pair_send.at[k, slot], pair_recv.at[k, slot],
                    ps_sem.at[k, slot], pr_sem.at[k, slot],
                    device_id=sibling, device_id_type=MESH,
                )
                copy.start()
                pair[k, slot] = copy
                waits.append(copy)
    kepts = []
    for off in range(1, n):
        copy = pltpu.make_async_remote_copy(
            kept_send.at[0], kept_recv.at[off - 1], ks_sem.at[off - 1], kr_sem.at[off - 1],
            device_id=peer({"dp": off}), device_id_type=MESH,
        )
        copy.start()
        kepts.append(copy)
        waits.append(copy)

    ring = {}
    for k in range(chunks):
        for slot in range(1, chips):
            target = chip_at(slot) * 2 + core
            mine = term(k, target)
            pair[k, slot].wait_recv()
            ring_send[k, slot - 1] = pair_recv[k, slot] + mine
            copy = pltpu.make_async_remote_copy(
                ring_send.at[k, slot - 1], ring_recv.at[k, slot - 1],
                rs_sem.at[k, slot - 1], rr_sem.at[k, slot - 1],
                device_id={"dp": target}, device_id_type=MESH,
            )
            copy.start()
            ring[k, slot] = copy
            waits.append(copy)

    count_row = kept_row
    for i, copy in enumerate(kepts):
        copy.wait_recv()
        count_row = count_row + kept_recv[i, :, 0:rows]
    inverse = 1.0 / jnp.maximum(as_column(count_row, rows), 1.0)

    for k in range(chunks):
        mine = term(k, me["dp"])
        pair[k, 0].wait_recv()
        total[k * part:(k + 1) * part, :] = pair_recv[k, 0] + mine

    steps = jnp.full((8, LANES), step_ref[0], jnp.int32)
    scale_m = (1.0 / (1.0 - int_power(0.9, steps)))[0:1, 0:1]
    scale_v = (1.0 / (1.0 - int_power(0.999, steps)))[0:1, 0:1]
    for copy in states:
        copy.wait()

    squares = jnp.zeros((8, LANES), jnp.float32)
    for k in range(chunks):
        at = slice(k * part, (k + 1) * part)
        value = total[at, :]
        for slot in range(1, chips):
            ring[k, slot].wait_recv()
            value = value + ring_recv[k, slot - 1]
        value = value * inverse[at]
        total[at, :] = value
        squares = squares + jnp.sum(
            (value * value).reshape(part // 8, 8, width // LANES, LANES), axis=(0, 2)
        )

    lane = lax.broadcasted_iota(jnp.int32, (1, LANES), 1)
    half = LANES // 2
    packed = jnp.sum(squares, axis=0, keepdims=True)
    packed = packed + pltpu.roll(packed, half, 1)
    packed = jnp.where(lane < half, packed, jnp.where(lane == half, dropped, 0.0))
    for axes, send, recv, s_sem, r_sem in zip(stages, red_sends, red_recvs, as_sems, ar_sems):
        send[0] = packed
        copies = []
        for i, off in enumerate(offsets_of(axes)):
            copy = pltpu.make_async_remote_copy(
                send.at[0], recv.at[i], s_sem.at[i], r_sem.at[i],
                device_id=peer(off), device_id_type=MESH,
            )
            copy.start()
            copies.append(copy)
            waits.append(copy)
        for i, copy in enumerate(copies):
            copy.wait_recv()
        for i in range(len(copies)):
            packed = packed + recv[i]
    square_sum = jnp.sum(jnp.where(lane < half, packed, 0.0), axis=1, keepdims=True)
    rms = jnp.sqrt(square_sum * (1.0 / entries))
    clip = jnp.minimum(1.0, 0.05 / (rms + 1e-06))

    for k in range(chunks):
        at = slice(k * part, (k + 1) * part)
        scaled = total[at, :] * clip
        new_m = 0.9 * m_buf[at, :] + 0.1 * scaled
        new_v = 0.999 * v_buf[at, :] + 0.001 * (scaled * scaled)
        weights = w_buf[at, :]
        direction = (new_m * scale_m) / (jnp.sqrt(new_v * scale_v) + 1e-08) + 0.1 * weights
        m_out[0, 0, at, :] = new_m
        v_out[0, 0, at, :] = new_v
        dir_out[0, 0, at, :] = direction
        w_out[0, 0, at, :] = weights - 0.001 * direction
    drop_out[0] = jnp.sum(jnp.where(lane == half, packed, 0.0)).astype(jnp.int32)

    for copy in waits:
        copy.wait_send()


def body(sizes, grad_parts, drop_flags, owner_order, step_count, master, moment_m, moment_v):
    n = sizes["dp"]
    chips = n // 2
    rows, columns = grad_parts.shape[-2:]
    width = master.shape[-1]
    chunks = rows // 8
    part = rows // chunks
    devices = n * sizes["tensor"] * sizes["pipe"]
    stages = [AXES] if devices <= DIRECT else [(axis,) for axis in AXES]
    peers = []
    for axes in stages:
        size = 1
        for axis in axes:
            size *= sizes[axis]
        peers.append(size - 1)
    entries = rows * columns * sizes["tensor"] * sizes["pipe"]
    padded = -(-rows // LANES) * LANES
    others = max(chips - 1, 1)
    f32 = jnp.float32
    dma = pltpu.SemaphoreType.DMA
    vmem = pl.BlockSpec(memory_space=pltpu.VMEM)
    smem = pl.BlockSpec(memory_space=pltpu.SMEM)
    hbm = pl.BlockSpec(memory_space=pl.ANY)
    state = jax.ShapeDtypeStruct(master.shape, f32)
    outs = pl.pallas_call(
        functools.partial(kernel, sizes, stages, entries, chunks),
        out_shape=(state, state, state, state, jax.ShapeDtypeStruct((1,), jnp.int32)),
        in_specs=[smem, smem, vmem, hbm, hbm, hbm, hbm],
        out_specs=(vmem, vmem, vmem, vmem, smem),
        scratch_shapes=[
            [pltpu.VMEM((part, columns), f32) for _ in range(chunks)],
            pltpu.VMEM((rows, width), f32),
            pltpu.VMEM((rows, width), f32),
            pltpu.VMEM((rows, width), f32),
            pltpu.VMEM((chunks, chips, part, width), f32),
            pltpu.VMEM((chunks, chips, part, width), f32),
            pltpu.VMEM((chunks, others, part, width), f32),
            pltpu.VMEM((chunks, others, part, width), f32),
            pltpu.VMEM((1, 1, padded), f32),
            pltpu.VMEM((n - 1, 1, padded), f32),
            pltpu.VMEM((rows, width), f32),
            [pltpu.VMEM((1, 1, LANES), f32) for _ in peers],
            [pltpu.VMEM((max(size, 1), 1, LANES), f32) for size in peers],
            dma((chunks,)),
            dma((3,)),
            dma((chunks, chips)),
            dma((chunks, chips)),
            dma((chunks, others)),
            dma((chunks, others)),
            dma((n - 1,)),
            dma((n - 1,)),
            [dma((max(size, 1),)) for size in peers],
            [dma((max(size, 1),)) for size in peers],
        ],
        compiler_params=pltpu.CompilerParams(collective_id=0, has_side_effects=True),
    )(
        owner_order, step_count.reshape(1), drop_flags.reshape(drop_flags.shape[-3:]),
        grad_parts, master, moment_m, moment_v,
    )
    return (*outs[:4], outs[4].reshape(()))


def solution(mesh):
    return jax.shard_map(
        functools.partial(body, dict(mesh.shape)),
        mesh=mesh,
        in_specs=(
            P("dp", "pipe", "tensor", None, None),
            P("dp", "pipe", "tensor", None),
            P(),
            P(),
            P("pipe", "tensor", None, "dp"),
            P("pipe", "tensor", None, "dp"),
            P("pipe", "tensor", None, "dp"),
        ),
        out_specs=(
            P("pipe", "tensor", None, "dp"),
            P("pipe", "tensor", None, "dp"),
            P("pipe", "tensor", None, "dp"),
            P("pipe", "tensor", None, "dp"),
            P(),
        ),
        check_vma=False,
    )
```

```python
import functools
import itertools
import jax
import jax.numpy as jnp
from jax import lax
from jax.experimental import pallas as pl
from jax.experimental.pallas import tpu as pltpu
from jax.sharding import PartitionSpec as P

AXES = ("dp", "tensor", "pipe")
MESH = pl.DeviceIdType.MESH
LANES = 128
DIRECT = 64
VMEM_MOST = 67043328


def as_column(row, rows):
    square = (rows, rows)
    diagonal = lax.broadcasted_iota(jnp.int32, square, 0) == lax.broadcasted_iota(jnp.int32, square, 1)
    return jnp.sum(jnp.where(diagonal, jnp.broadcast_to(row, square), 0.0), axis=1, keepdims=True)


def int_power(base, exponent):
    result = jnp.ones(exponent.shape, jnp.float32)
    square = jnp.full(exponent.shape, base, jnp.float32)
    for bit in range(31):
        result = jnp.where((exponent >> bit) & 1 == 1, result * square, result)
        square = square * square
    return result


def kernel(
    sizes, stages, chunks,
    order_hbm, flags_hbm, grad_hbm,
    total, norm_out,
    order_ref, flags_ref, g_bufs, pair_send, pair_recv, ring_send, ring_recv,
    kept_send, kept_recv, red_sends, red_recvs,
    o_sem, g_sem, ps_sem, pr_sem, rs_sem, rr_sem, ks_sem, kr_sem, as_sems, ar_sems,
):
    n = sizes["dp"]
    chips = n // 2
    rows, width = total.shape
    part = rows // chunks
    me = {axis: lax.axis_index(axis) for axis in AXES}
    chip, core = lax.div(me["dp"], 2), lax.rem(me["dp"], 2)

    def peer(offsets):
        return {axis: lax.rem(me[axis] + off, sizes[axis]) for axis, off in offsets.items()}

    def offsets_of(axes):
        ranges = [range(sizes[axis]) for axis in axes]
        return [dict(zip(axes, offs)) for offs in itertools.product(*ranges) if any(offs)]

    small = [
        pltpu.make_async_copy(order_hbm, order_ref, o_sem.at[0]),
        pltpu.make_async_copy(flags_hbm, flags_ref, o_sem.at[1]),
    ]
    for copy in small:
        copy.start()
    loads = []
    for k in range(chunks):
        copy = pltpu.make_async_copy(grad_hbm.at[0, 0, 0, pl.ds(k * part, part)], g_bufs[k], g_sem.at[k])
        copy.start()
        loads.append(copy)

    barrier = pltpu.get_barrier_semaphore()
    friends = [tuple(sorted(off.items())) for axes in stages for off in offsets_of(axes)]
    friends += [tuple(sorted(off.items())) for off in offsets_of(("dp",))]
    full = [tuple(sorted({**dict.fromkeys(AXES, 0), **dict(off)}.items())) for off in friends]
    full = list(dict.fromkeys(full))
    for off in full:
        pl.semaphore_signal(barrier, inc=1, device_id=peer(dict(off)), device_id_type=MESH)

    for copy in small:
        copy.wait()
    flags_row = flags_ref[0].astype(jnp.float32)
    kept_row = 1.0 - flags_row
    kept = as_column(kept_row, rows)
    kept_send[0, :, 0:rows] = kept_row
    dropped = jnp.sum(flags_row, axis=1, keepdims=True)

    def chip_at(slot):
        return lax.rem(chip + slot, chips)

    def term(k, owner):
        block = order_ref[owner]
        picked = None
        for b in range(n):
            weight = (1 - jnp.minimum(jnp.maximum(block - b, b - block), 1)).astype(jnp.float32)
            piece = g_bufs[k][:, b * width:(b + 1) * width] * weight
            picked = piece if picked is None else picked + piece
        return picked * kept[k * part:(k + 1) * part]

    slots = list(range(1, chips)) + [0]
    for k in range(chunks):
        loads[k].wait()
        for slot in slots:
            pair_send[k, slot] = term(k, chip_at(slot) * 2 + 1 - core)

    pl.semaphore_wait(barrier, len(full))

    sibling = {"dp": chip * 2 + 1 - core}
    pair, waits = {}, []
    for group in (slots[:-1], slots[-1:]):
        for k in range(chunks):
            for slot in group:
                copy = pltpu.make_async_remote_copy(
                    pair_send.at[k, slot], pair_recv.at[k, slot],
                    ps_sem.at[k, slot], pr_sem.at[k, slot],
                    device_id=sibling, device_id_type=MESH,
                )
                copy.start()
                pair[k, slot] = copy
                waits.append(copy)
    kepts = []
    for off in range(1, n):
        copy = pltpu.make_async_remote_copy(
            kept_send.at[0], kept_recv.at[off - 1], ks_sem.at[off - 1], kr_sem.at[off - 1],
            device_id=peer({"dp": off}), device_id_type=MESH,
        )
        copy.start()
        kepts.append(copy)
        waits.append(copy)

    ring = {}
    for k in range(chunks):
        for slot in range(1, chips):
            target = chip_at(slot) * 2 + core
            mine = term(k, target)
            pair[k, slot].wait_recv()
            ring_send[k, slot - 1] = pair_recv[k, slot] + mine
            copy = pltpu.make_async_remote_copy(
                ring_send.at[k, slot - 1], ring_recv.at[k, slot - 1],
                rs_sem.at[k, slot - 1], rr_sem.at[k, slot - 1],
                device_id={"dp": target}, device_id_type=MESH,
            )
            copy.start()
            ring[k, slot] = copy
            waits.append(copy)

    count_row = kept_row
    for i, copy in enumerate(kepts):
        copy.wait_recv()
        count_row = count_row + kept_recv[i, :, 0:rows]
    inverse = 1.0 / jnp.maximum(as_column(count_row, rows), 1.0)

    for k in range(chunks):
        mine = term(k, me["dp"])
        pair[k, 0].wait_recv()
        total[k * part:(k + 1) * part, :] = pair_recv[k, 0] + mine

    squares = jnp.zeros((8, LANES), jnp.float32)
    for k in range(chunks):
        at = slice(k * part, (k + 1) * part)
        value = total[at, :]
        for slot in range(1, chips):
            ring[k, slot].wait_recv()
            value = value + ring_recv[k, slot - 1]
        value = value * inverse[at]
        total[at, :] = value
        squares = squares + jnp.sum(
            (value * value).reshape(part // 8, 8, width // LANES, LANES), axis=(0, 2)
        )

    lane = lax.broadcasted_iota(jnp.int32, (1, LANES), 1)
    half = LANES // 2
    packed = jnp.sum(squares, axis=0, keepdims=True)
    packed = packed + pltpu.roll(packed, half, 1)
    packed = jnp.where(lane < half, packed, jnp.where(lane == half, dropped, 0.0))
    for axes, send, recv, s_sem, r_sem in zip(stages, red_sends, red_recvs, as_sems, ar_sems):
        send[0] = packed
        copies = []
        for i, off in enumerate(offsets_of(axes)):
            copy = pltpu.make_async_remote_copy(
                send.at[0], recv.at[i], s_sem.at[i], r_sem.at[i],
                device_id=peer(off), device_id_type=MESH,
            )
            copy.start()
            copies.append(copy)
            waits.append(copy)
        for i, copy in enumerate(copies):
            copy.wait_recv()
        for i in range(len(copies)):
            packed = packed + recv[i]
    norm_out[0] = jnp.sum(jnp.where(lane < half, packed, 0.0))
    norm_out[1] = jnp.sum(jnp.where(lane == half, packed, 0.0))

    for copy in waits:
        copy.wait_send()


def update(
    entries, chunks, step_ref, norm_ref, grad_ref, w_ref, m_ref, v_ref,
    w_out, m_out, v_out, dir_out, drop_out, bufs, sems,
):
    rows, width = grad_ref.shape
    part = rows // chunks
    steps = jnp.full((8, LANES), step_ref[...], jnp.int32)
    scale_m = (1.0 / (1.0 - int_power(0.9, steps)))[0:1, 0:1]
    scale_v = (1.0 / (1.0 - int_power(0.999, steps)))[0:1, 0:1]
    rms = jnp.sqrt(jnp.full((8, LANES), norm_ref[0], jnp.float32) * (1.0 / entries))[0:1, 0:1]
    clip = jnp.minimum(1.0, 0.05 / (rms + 1e-06))
    copies = []
    for k in range(chunks):
        at = slice(k * part, (k + 1) * part)
        scaled = grad_ref[at, :] * clip
        new_m = 0.9 * m_ref[0, 0, at, :] + 0.1 * scaled
        new_v = 0.999 * v_ref[0, 0, at, :] + 0.001 * (scaled * scaled)
        weights = w_ref[0, 0, at, :]
        direction = (new_m * scale_m) / (jnp.sqrt(new_v * scale_v) + 1e-08) + 0.1 * weights
        values = (weights - 0.001 * direction, new_m, new_v, direction)
        for i, (value, out) in enumerate(zip(values, (w_out, m_out, v_out, dir_out))):
            bufs[i, at, :] = value
            copy = pltpu.make_async_copy(bufs.at[i, pl.ds(k * part, part)], out.at[0, 0, pl.ds(k * part, part)], sems.at[k, i])
            copy.start()
            copies.append(copy)
    drop_out[0] = norm_ref[1].astype(jnp.int32)
    for copy in copies:
        copy.wait()


def body(sizes, grad_parts, drop_flags, owner_order, step_count, master, moment_m, moment_v):
    n = sizes["dp"]
    chips = n // 2
    rows, columns = grad_parts.shape[-2:]
    width = master.shape[-1]
    chunks = rows // 8
    part = rows // chunks
    devices = n * sizes["tensor"] * sizes["pipe"]
    stages = [AXES] if devices <= DIRECT else [(axis,) for axis in AXES]
    peers = []
    for axes in stages:
        size = 1
        for axis in axes:
            size *= sizes[axis]
        peers.append(size - 1)
    entries = rows * columns * sizes["tensor"] * sizes["pipe"]
    padded = -(-rows // LANES) * LANES
    others = max(chips - 1, 1)
    f32 = jnp.float32
    dma = pltpu.SemaphoreType.DMA
    vmem = pl.BlockSpec(memory_space=pltpu.VMEM)
    smem = pl.BlockSpec(memory_space=pltpu.SMEM)
    hbm = pl.BlockSpec(memory_space=pltpu.HBM)
    state = jax.ShapeDtypeStruct(master.shape, f32)
    room = rows * columns * 4 - (64 << 10)
    grad, norm = pl.pallas_call(
        functools.partial(kernel, sizes, stages, chunks),
        out_shape=(
            jax.ShapeDtypeStruct((rows, width), f32),
            jax.ShapeDtypeStruct((2,), f32),
        ),
        in_specs=[hbm, hbm, hbm],
        out_specs=(vmem, smem),
        scratch_shapes=[
            pltpu.SMEM((n,), jnp.int32),
            pltpu.VMEM((1, 1, rows), jnp.int32),
            [pltpu.VMEM((part, columns), f32) for _ in range(chunks)],
            pltpu.VMEM((chunks, chips, part, width), f32),
            pltpu.VMEM((chunks, chips, part, width), f32),
            pltpu.VMEM((chunks, others, part, width), f32),
            pltpu.VMEM((chunks, others, part, width), f32),
            pltpu.VMEM((1, 1, padded), f32),
            pltpu.VMEM((n - 1, 1, padded), f32),
            [pltpu.VMEM((1, 1, LANES), f32) for _ in peers],
            [pltpu.VMEM((max(size, 1), 1, LANES), f32) for size in peers],
            dma((2,)),
            dma((chunks,)),
            dma((chunks, chips)),
            dma((chunks, chips)),
            dma((chunks, others)),
            dma((chunks, others)),
            dma((n - 1,)),
            dma((n - 1,)),
            [dma((max(size, 1),)) for size in peers],
            [dma((max(size, 1),)) for size in peers],
        ],
        compiler_params=pltpu.CompilerParams(
            collective_id=0, has_side_effects=True, vmem_limit_bytes=VMEM_MOST - room
        ),
        cost_estimate=pl.CostEstimate(
            flops=8 * rows * columns, bytes_accessed=20 * rows * columns * 4, transcendentals=0
        ),
    )(owner_order, drop_flags.reshape(drop_flags.shape[-3:]), grad_parts)
    outs = pl.pallas_call(
        functools.partial(update, entries, chunks),
        out_shape=(state, state, state, state, jax.ShapeDtypeStruct((1,), jnp.int32)),
        in_specs=[smem, smem, vmem, vmem, vmem, vmem],
        out_specs=(hbm, hbm, hbm, hbm, smem),
        scratch_shapes=[pltpu.VMEM((4, rows, width), f32), dma((chunks, 4))],
        compiler_params=pltpu.CompilerParams(vmem_limit_bytes=VMEM_MOST - 7 * rows * width),
        cost_estimate=pl.CostEstimate(
            flops=20 * rows * width, bytes_accessed=8 * rows * width * 4, transcendentals=0
        ),
    )(step_count, norm, grad, master, moment_m, moment_v)
    return (*outs[:4], outs[4].reshape(()))


def solution(mesh):
    return jax.shard_map(
        functools.partial(body, dict(mesh.shape)),
        mesh=mesh,
        in_specs=(
            P("dp", "pipe", "tensor", None, None),
            P("dp", "pipe", "tensor", None),
            P(),
            P(),
            P("pipe", "tensor", None, "dp"),
            P("pipe", "tensor", None, "dp"),
            P("pipe", "tensor", None, "dp"),
        ),
        out_specs=(
            P("pipe", "tensor", None, "dp"),
            P("pipe", "tensor", None, "dp"),
            P("pipe", "tensor", None, "dp"),
            P("pipe", "tensor", None, "dp"),
            P(),
        ),
        check_vma=False,
    )
```
